32 devices in a mesh: user: 8 (over z, x), pos: 4 (over y, core).
Axes of the slice: x: 2, y: 2, z: 4, core: 2. Of those that a mesh axis runs over, the one named last changes fastest.
Arguments:
- events: bfloat16 [8192, 256], P('user'), may hold values from -6 to 6
- owners: int32 [8192], P('user'), may hold values from 0 to 15, as said below
- offsets: int32 [8192], P('user'), may hold values from 0 to 2047, as said below
- w_key: bfloat16 [256, 256], replicated, may hold values from -0.375 to 0.375
- w_value: bfloat16 [256, 256], replicated, may hold values from -0.375 to 0.375
- cache_keys: bfloat16 [16, 6144, 256], P('user', 'pos'), may hold values from -7 to 7
- cache_values: bfloat16 [16, 6144, 256], P('user', 'pos'), may hold values from -6 to 6
- hist_len: int32 [16], P('user'), may hold values from 8 to 4096
- active: int32 [16], P('user'), may hold values 0 or 1
- candidates: bfloat16 [16, 1024, 256], P('user', 'pos'), may hold values from -100 to 100
Outputs:
- new_keys: bfloat16 [16, 6144, 256], P('user', 'pos')
- new_values: bfloat16 [16, 6144, 256], P('user', 'pos')
- attended: bfloat16 [16, 1024, 256], P('user', 'pos')
The draws below stay inside these ranges and needn't reach their ends.
Inputs may be any that keep to these rules, and one draw needn't show every extreme that they name: Among the events of one aligned block of 1024 (one index of user), at most 256 have owners among the users t * 2 to t * 2 + 1, for every t; in every draw some t receives exactly 256 from every block, and all those events belong to one user of that t. offsets[e] is the number of events before e, in the order of the array, that have the same owner as e.
All inputs are finite; a program needn't handle non-finite values. No bound on the sum of `active` on one device may be relied on, other than what follows from the above.
Results may differ from the reference program's by a relative error of at most 0.0067.
Values may be sent and summed in bfloat16 or wider, within the bound.
A program may use at most 128 MiB of HBM per device.

```python
import jax
import jax.numpy as jnp
from jax import lax

U_DEV = 2
P_DEV = 1536
EV_DEV = 1024
D = 256
F = 256
CAND = 1024
USERS = 16
HIST = 6144
EVENTS = 8192
CAP = 256
N_POS = 4


def key_head(key):
    head = jnp.clip(jax.random.normal(jax.random.fold_in(key, 7002), (USERS, 6, D), jnp.float32), -6.0, 6.0)
    return head


def draw_cache_keys(key, part):
    rows = jnp.clip(jax.random.normal(jax.random.fold_in(key, 7001), (USERS, HIST, D), jnp.float32), -6.0, 6.0)
    head = key_head(key)
    rows = rows.at[:, :6].set(head)
    return rows.astype(jnp.bfloat16)


def draw_candidates(key, part):
    values = jnp.clip(jax.random.normal(jax.random.fold_in(key, 7003), (USERS, CAND, D), jnp.float32), -6.0, 6.0)
    return values.astype(jnp.bfloat16)


def routing(key):
    groups = USERS // U_DEV
    width = groups * CAP
    splits = jax.random.split(jax.random.fold_in(key, 7101), groups)

    def shuffle(single):
        return jax.random.permutation(single, width).astype(jnp.int32)
    perms = jax.vmap(shuffle)(splits)
    full = jax.random.randint(jax.random.fold_in(key, 7102), (), 0, groups).astype(jnp.int32)
    column = jnp.arange(width, dtype=jnp.int32) // CAP
    score = jnp.where(column[None, :] == full, perms - width, perms)
    chosen = jnp.argsort(score, axis=1)[:, :EV_DEV].astype(jnp.int32)
    dest = chosen // CAP
    local = jax.random.randint(jax.random.fold_in(key, 7103), (groups, EV_DEV), 0, U_DEV).astype(jnp.int32)
    heavy = jax.random.randint(jax.random.fold_in(key, 7104), (), 0, U_DEV).astype(jnp.int32)
    local = jnp.where(dest == full, heavy, local).astype(jnp.int32)
    owners = (dest * U_DEV + local).reshape(-1).astype(jnp.int32)
    order_all = jnp.argsort(owners, stable=True).astype(jnp.int32)
    sorted_owner = owners[order_all]
    start = jnp.searchsorted(sorted_owner, sorted_owner, side='left').astype(jnp.int32)
    rank_sorted = jnp.arange(EVENTS, dtype=jnp.int32) - start
    offsets = jnp.zeros((EVENTS,), jnp.int32).at[order_all].set(rank_sorted)
    return (owners, offsets)


def draw_owners(key, part):
    return routing(key)[0]


def draw_offsets(key, part):
    return routing(key)[1]


def touch_ends(result, key, low, top_value):
    longest = result.shape.index(max(result.shape))
    spots = []
    for shift in (0, 1):
        where = [jax.random.randint(jax.random.fold_in(key, axis), (), 0, length) for axis, length in enumerate(result.shape)]
        where[longest] = (where[longest] + shift) % result.shape[longest]
        spots.append(tuple(where))
    return result.at[spots[0]].set(low).at[spots[1]].set(top_value)


def block_scale(rng, extent, cuts, low, top_value):
    def one(dim, blocks):
        steps = jax.random.uniform(jax.random.fold_in(jax.random.fold_in(rng, 6), dim), (blocks,), jnp.float32, low / len(cuts), top_value / len(cuts))
        return jnp.repeat(jnp.exp(steps), extent[dim] // blocks).reshape((-1,) + (1,) * (len(extent) - dim - 1))

    loudness = one(*cuts[0])
    for cut in cuts[1:]:
        loudness = loudness * one(*cut)
    return loudness


def normal_values(rng, extent, spread, limit, pieces=(), kind=jnp.bfloat16):
    loudness = block_scale(rng, extent, pieces, -0.22, 0.18) if pieces else 1.0
    values = jax.random.normal(rng, extent, jnp.float32) * spread * loudness
    return jnp.minimum(jnp.maximum(values, -limit), limit).astype(kind)


def setup_inputs(seed: int = 0) -> dict:
    key_list = jax.random.split(jax.random.key(seed), 11)
    return {
        "events": normal_values(key_list[0], (EVENTS, F), 1.0, 6.0, ((0, 8),)),
        "owners": draw_owners(jax.random.fold_in(key_list[10], 71), 0),
        "offsets": draw_offsets(jax.random.fold_in(key_list[10], 71), 0),
        "w_key": normal_values(key_list[3], (F, D), F ** -0.5, 0.375),
        "w_value": normal_values(key_list[4], (F, D), F ** -0.5, 0.375),
        "cache_keys": draw_cache_keys(jax.random.fold_in(key_list[10], 71), 0),
        "cache_values": normal_values(key_list[6], (USERS, HIST, D), 1.0, 6.0, ((0, 8), (1, 4))),
        "hist_len": touch_ends(jax.random.randint(key_list[7], (USERS,), 8, HIST - 2 * EV_DEV + 1), jax.random.fold_in(key_list[7], 1), 8, HIST - 2 * EV_DEV).astype(jnp.int32),
        "active": touch_ends((jax.random.randint(key_list[8], (USERS,), 0, 4) < 3).astype(jnp.int32), jax.random.fold_in(key_list[8], 1), 0, 1),
        "candidates": draw_candidates(jax.random.fold_in(key_list[10], 71), 0),
    }


def reference(events, owners, offsets, w_key, w_value, cache_keys, cache_values, hist_len, active, candidates):
    new_k = jnp.dot(events, w_key, preferred_element_type=jnp.float32).astype(jnp.bfloat16)
    new_v = jnp.dot(events, w_value, preferred_element_type=jnp.float32).astype(jnp.bfloat16)
    target = (hist_len[owners] + offsets).astype(jnp.int32)
    new_keys = cache_keys.at[owners, target].set(new_k)
    new_values = cache_values.at[owners, target].set(new_v)
    counts = jax.ops.segment_sum(jnp.ones_like(owners), owners, num_segments=USERS).astype(jnp.int32)
    limits = (hist_len + counts).astype(jnp.int32)
    scale = D ** -0.5

    def per_user(pack):
        query, key_rows, value_rows, bound, flag = pack
        scores = jnp.dot(query, key_rows.T, preferred_element_type=jnp.float32) * scale
        scores = scores.reshape(CAND, N_POS, P_DEV)
        position = jnp.arange(HIST, dtype=jnp.int32).reshape(N_POS, P_DEV)
        valid = (position < bound)[None]
        masked = jnp.where(valid, scores, jnp.float32(-1e30))
        block_max = jnp.max(masked, axis=2)
        expo = jnp.where(valid, jnp.exp(masked - block_max[:, :, None]), jnp.float32(0.0))
        block_sum = jnp.sum(expo, axis=2)
        weights = expo.astype(jnp.bfloat16)
        parts = jnp.einsum("cbp,bpd->cbd", weights.astype(jnp.float32),
                           value_rows.reshape(N_POS, P_DEV, D).astype(jnp.float32))
        top = jnp.max(block_max, axis=1)
        factor = jnp.exp(block_max - top[:, None])
        total = jnp.sum(block_sum * factor, axis=1)
        acc = jnp.sum(parts * factor[:, :, None], axis=1)
        return (acc / total[:, None] * flag).astype(jnp.bfloat16)

    attended = lax.map(per_user, (candidates, new_keys, new_values, limits, active.astype(jnp.float32)))
    return new_keys, new_values, attended
```

```python
import functools
import math

import jax
import jax.numpy as jnp
from jax import lax
from jax.experimental import pallas as pl
from jax.experimental.pallas import tpu as pltpu
from jax.sharding import PartitionSpec as P

MESH = pl.DeviceIdType.MESH
NT = (((1,), (1,)), ((), ()))
TAIL = 16


def pos_peers():
    p = lax.axis_index("pos")
    near = p + 1 - 2 * lax.rem(p, 2)
    far = lax.rem(p + 2, 4)
    return p, near, far


def exchange_kernel(
    groups, blocks, users_here, cap,
    events_ref, owners_ref, cand_ref,
    rows_ref, queries_ref,
    packed, local_sem, a2a_send, a2a_recv, hop_send, hop_recv, q_send, q_recv,
):
    me = lax.axis_index("user")
    p, near, far = pos_peers()
    count = groups // blocks
    first = lax.rem(p - me + blocks * groups, blocks)
    far_first = lax.rem(far - me + blocks * groups, blocks)
    peers = [first + blocks * k for k in range(count)]

    barrier = pltpu.get_barrier_semaphore()
    for peer in (near, far):
        pl.semaphore_signal(barrier, inc=1, device_id={"pos": peer}, device_id_type=MESH)
    for peer in peers:
        @pl.when(peer != me)
        def _():
            pl.semaphore_signal(barrier, inc=1, device_id={"user": peer}, device_id_type=MESH)
    itself = (lax.rem(me, blocks) == first).astype(jnp.int32)
    pl.semaphore_wait(barrier, 2 + count - itself)

    def hop(ref_src, ref_dst, send, recv, peer):
        return pltpu.make_async_remote_copy(
            src_ref=ref_src, dst_ref=ref_dst, send_sem=send, recv_sem=recv,
            device_id={"pos": peer}, device_id_type=MESH,
        )

    q_far = hop(cand_ref, queries_ref.at[p], q_send.at[0], q_recv.at[0], far)
    q_far.start()
    q_near = hop(cand_ref, queries_ref.at[p], q_send.at[1], q_recv.at[1], near)
    q_near.start()
    q_own = pltpu.make_async_copy(cand_ref, queries_ref.at[p], local_sem.at[count])
    q_own.start()

    per_event = events_ref.shape[0]
    width = events_ref.shape[1]
    users = groups * users_here
    owner = owners_ref[...]
    user_id = lax.broadcasted_iota(jnp.int32, (users, per_event), 0)
    same = (user_id == owner).astype(jnp.float32)
    before = (
        lax.broadcasted_iota(jnp.int32, (per_event, per_event), 0)
        <= lax.broadcasted_iota(jnp.int32, (per_event, per_event), 1)
    ).astype(jnp.float32).astype(jnp.bfloat16)
    ranks = jnp.dot(same.astype(jnp.bfloat16), before, preferred_element_type=jnp.float32)
    counts = jnp.sum(same, axis=1, keepdims=True)
    dest = owner // users_here
    earlier = (user_id >= dest * users_here) & (user_id < owner)
    slot = jnp.sum(jnp.where(earlier, counts, 0.0) + same * ranks, axis=0, keepdims=True) - 1.0
    slot = slot.astype(jnp.int32)
    slot_id = lax.broadcasted_iota(jnp.int32, (cap, per_event), 0)
    lane = lax.broadcasted_iota(jnp.int32, (users, width), 1)
    lane_user = lax.broadcasted_iota(jnp.int32, (users, width), 0)

    def a2a(k, peer, slot):
        return pltpu.make_async_remote_copy(
            src_ref=packed.at[k], dst_ref=rows_ref.at[me],
            send_sem=a2a_send.at[k], recv_sem=a2a_recv.at[slot],
            device_id={"user": peer}, device_id_type=MESH,
        )

    def own(k):
        return pltpu.make_async_copy(packed.at[k], rows_ref.at[me], local_sem.at[k])

    for k, peer in enumerate(peers):
        wanted = jnp.where(dest == peer, slot, -1)
        pick = (wanted == slot_id).astype(jnp.float32).astype(jnp.bfloat16)
        packed[k, :cap, :] = jnp.dot(
            pick, events_ref[...], preferred_element_type=jnp.float32
        ).astype(jnp.bfloat16)
        row = jnp.sum(
            jnp.where(lane_user == lane + peer * users_here, counts, 0.0), axis=0, keepdims=True
        )
        packed[k, cap:, :] = jnp.broadcast_to(row, (TAIL, width)).astype(jnp.bfloat16)

        @pl.when(peer != me)
        def _():
            a2a(k, peer, me // blocks).start()

        @pl.when(peer == me)
        def _():
            own(k).start()

    def forward(stage, k, start, peer):
        block = rows_ref.at[start + blocks * k]
        return hop(block, block, hop_send.at[stage, k], hop_recv.at[stage, k], peer)

    q_far.wait_recv()
    q_across = hop(queries_ref.at[far], queries_ref.at[far], q_send.at[2], q_recv.at[2], near)
    q_across.start()
    for k, peer in enumerate(peers):
        @pl.when(peer != me)
        def _():
            a2a(k, peer, k).wait_recv()

        @pl.when(peer == me)
        def _():
            own(k).wait()

        forward(0, k, first, far).start()
        forward(1, k, first, near).start()
    for k in range(count):
        forward(0, k, first, far).wait_recv()
        forward(2, k, far_first, near).start()
    for k in range(count):
        forward(1, k, first, near).wait_recv()
        forward(2, k, far_first, near).wait_recv()
    q_near.wait_recv()
    q_across.wait_recv()
    q_own.wait()
    q_far.wait_send()
    q_near.wait_send()
    q_across.wait_send()
    for k, peer in enumerate(peers):
        @pl.when(peer != me)
        def _():
            a2a(k, peer, k).wait_send()

        forward(0, k, first, far).wait_send()
        forward(1, k, first, near).wait_send()
        forward(2, k, far_first, near).wait_send()


def attend_kernel(
    groups, cap, scale,
    count_ref, hist_ref, rows_ref, weight_ref, keys_ref, values_ref, queries_ref,
    new_keys_ref, new_values_ref, part_ref, stat_ref,
    made, fresh, acc, top, total, eye,
):
    user = pl.program_id(0)
    step = pl.program_id(1)
    steps = pl.num_programs(1)
    rows = keys_ref.shape[1]
    width = keys_ref.shape[2]
    quarters, quarter = queries_ref.shape[0], queries_ref.shape[2]
    users_here = hist_ref.shape[0]

    @pl.when((user == 0) & (step == 0))
    def _():
        def project(g, carry):
            made[g] = jnp.dot(
                rows_ref[g, :cap, :], weight_ref[...], preferred_element_type=jnp.float32
            ).astype(jnp.bfloat16)
            return carry

        lax.fori_loop(0, groups, project, 0)
        eye[...] = (
            lax.broadcasted_iota(jnp.int32, (width, width), 0)
            == lax.broadcasted_iota(jnp.int32, (width, width), 1)
        ).astype(jnp.float32).astype(jnp.bfloat16)

    @pl.when(step == 0)
    def _():
        acc[...] = jnp.zeros_like(acc)
        top[...] = jnp.full_like(top, -1e30)
        total[...] = jnp.zeros_like(total)

    origin = (lax.axis_index("pos") * steps + step) * rows
    start = hist_ref[user] - origin
    limit = lax.fori_loop(0, groups, lambda g, n: n + count_ref[g, user], start)
    touched = (limit > 0) & (start < rows) & (limit > start)
    new_keys_ref[...] = keys_ref[...]
    new_values_ref[...] = values_ref[...]

    @pl.when(touched)
    def _():
        fresh[...] = jnp.zeros_like(fresh)
        gap = lax.broadcasted_iota(jnp.int32, (rows, cap), 1) - lax.broadcasted_iota(
            jnp.int32, (rows, cap), 0
        )
        slot = lax.broadcasted_iota(jnp.int32, (rows, cap), 1)

        def place(g, at):
            size = count_ref[g, user]

            @pl.when((size > 0) & (at < rows) & (at + size > 0))
            def _():
                low = lax.fori_loop(0, user, lambda j, n: n + count_ref[g, j], 0)
                pick = (gap == low - at) & (slot >= low) & (slot < low + size)
                fresh[...] += jnp.dot(
                    pick.astype(jnp.float32).astype(jnp.bfloat16), made[g],
                    preferred_element_type=jnp.float32,
                )

            return at + size

        lax.fori_loop(0, groups, place, start)
        row = lax.broadcasted_iota(jnp.int32, (rows, width), 0)
        inside = (row >= start) & (row < limit)
        new_keys_ref[0] = jnp.where(
            inside, fresh[:, :width], keys_ref[0].astype(jnp.float32)
        ).astype(jnp.bfloat16)
        new_values_ref[0] = jnp.where(
            inside, fresh[:, width:], values_ref[0].astype(jnp.float32)
        ).astype(jnp.bfloat16)

    @pl.when(limit > 0)
    def _():
        keys = new_keys_ref[0]
        flipped = lax.dot_general(
            eye[...], new_values_ref[0], NT, preferred_element_type=jnp.float32
        ).astype(jnp.bfloat16)
        valid = lax.broadcasted_iota(jnp.int32, (rows, quarter), 0) < limit
        for c in range(quarters):
            scores = lax.dot_general(
                keys, queries_ref[c, 0], NT, preferred_element_type=jnp.float32
            ) * (scale * math.log2(math.e))
            scores = jnp.where(valid, scores, -1e30)
            old = top[c : c + 1]
            high = jnp.maximum(old, jnp.max(scores, axis=0, keepdims=True))
            expo = jnp.exp2(scores - high)
            shrink = jnp.exp2(old - high)
            top[c : c + 1] = high
            total[c : c + 1] = total[c : c + 1] * shrink + jnp.sum(expo, axis=0, keepdims=True)
            acc[c] = acc[c] * shrink + jnp.dot(
                flipped, expo.astype(jnp.bfloat16), preferred_element_type=jnp.float32
            )

    @pl.when(step == steps - 1)
    def _():
        part_ref[:, 0] = acc[...].astype(jnp.bfloat16)
        for c in range(quarters):
            stat_ref[c, 0] = jnp.concatenate(
                [
                    jnp.broadcast_to(top[c : c + 1], (4, quarter)),
                    jnp.broadcast_to(total[c : c + 1], (4, quarter)),
                ],
                axis=0,
            )


def combine_kernel(
    part_ref, stat_ref, active_ref, out_ref,
    near_part, near_stat, send_part, send_stat, far_part, far_stat,
    near_send, near_recv, far_send, far_recv,
):
    p, near, far = pos_peers()
    low = lax.rem(p, 2)
    high = p // 2
    users_here = part_ref.shape[1]
    barrier = pltpu.get_barrier_semaphore()
    for peer in (near, far):
        pl.semaphore_signal(barrier, inc=1, device_id={"pos": peer}, device_id_type=MESH)
    pl.semaphore_wait(barrier, 2)

    def copies(src_part, src_stat, dst_part, dst_stat, send, recv, n, peer):
        return [
            pltpu.make_async_remote_copy(
                src_ref=src, dst_ref=dst, send_sem=send.at[i, n], recv_sem=recv.at[i, n],
                device_id={"pos": peer}, device_id_type=MESH,
            )
            for i, (src, dst) in enumerate(((src_part, dst_part), (src_stat, dst_stat)))
        ]

    theirs = (2 * (1 - high) + low, p)
    first = {}
    for h, quarter in enumerate((2 * (1 - high) + 1 - low, near)):
        for u in range(users_here):
            first[h, u] = copies(
                part_ref.at[quarter, u], stat_ref.at[quarter, u],
                near_part.at[h, u], near_stat.at[h, u],
                near_send, near_recv, h * users_here + u, near,
            )
            for copy in first[h, u]:
                copy.start()

    def merge(a_stat, a_part, b_stat, b_part):
        a_top, b_top = a_stat[0:1], b_stat[0:1]
        top = jnp.maximum(a_top, b_top)
        a_factor = jnp.exp2(a_top - top)
        b_factor = jnp.exp2(b_top - top)
        total = a_stat[4:5] * a_factor + b_stat[4:5] * b_factor
        part = a_part.astype(jnp.float32) * a_factor + b_part.astype(jnp.float32) * b_factor
        return top, total, part

    def local(h, u):
        for copy in first[h, u]:
            copy.wait_recv()
        return merge(
            stat_ref[theirs[h], u], part_ref[theirs[h], u], near_stat[h, u], near_part[h, u]
        )

    second = []
    for u in range(users_here):
        top, total, part = local(0, u)
        send_part[u] = part.astype(jnp.bfloat16)
        send_stat[u] = jnp.concatenate(
            [jnp.broadcast_to(top, (4,) + top.shape[1:]), jnp.broadcast_to(total, (4,) + top.shape[1:])],
            axis=0,
        )
        second.append(
            copies(
                send_part.at[u], send_stat.at[u], far_part.at[u], far_stat.at[u],
                far_send, far_recv, u, far,
            )
        )
        for copy in second[u]:
            copy.start()
    kept = [local(1, u) for u in range(users_here)]
    for u in range(users_here):
        top, total, part = kept[u]
        for copy in second[u]:
            copy.wait_recv()
        other = far_stat[u]
        new_top = jnp.maximum(top, other[0:1])
        mine = jnp.exp2(top - new_top)
        theirs_factor = jnp.exp2(other[0:1] - new_top)
        total = total * mine + other[4:5] * theirs_factor
        flag = active_ref[u].astype(jnp.float32)
        inverse = flag / total
        whole = part * (mine * inverse) + far_part[u].astype(jnp.float32) * (theirs_factor * inverse)
        out_ref[u] = whole.T.astype(jnp.bfloat16)
    for group in list(first.values()) + second:
        for copy in group:
            copy.wait_send()


def on_device(
    events, owners, offsets, w_key, w_value, cache_keys, cache_values, hist_len, active, candidates
):
    groups = lax.axis_size("user")
    blocks = lax.axis_size("pos")
    users_here, block_rows, width = cache_keys.shape
    per_event, features = events.shape
    cap = 2 * per_event // groups
    quarter = candidates.shape[1]
    count = groups // blocks
    vmem = pl.BlockSpec(memory_space=pltpu.VMEM)
    smem = pl.BlockSpec(memory_space=pltpu.SMEM)
    dma = pltpu.SemaphoreType.DMA
    bf16, f32 = jnp.bfloat16, jnp.float32

    rows, queries = pl.pallas_call(
        functools.partial(exchange_kernel, groups, blocks, users_here, cap),
        out_shape=(
            jax.ShapeDtypeStruct((groups, cap + TAIL, features), bf16),
            jax.ShapeDtypeStruct((blocks, users_here, quarter, width), bf16),
        ),
        in_specs=[vmem] * 3,
        out_specs=(vmem, vmem),
        scratch_shapes=[
            pltpu.VMEM((count, cap + TAIL, features), bf16),
            dma((count + 1,)), dma((count,)), dma((count,)),
            dma((3, count)), dma((3, count)), dma((3,)), dma((3,)),
        ],
        compiler_params=pltpu.CompilerParams(collective_id=0, has_side_effects=True),
        name="exchange",
    )(events, owners.reshape(1, per_event), candidates)

    counts = rows[:, cap, :users_here].astype(jnp.int32)
    weights = jnp.concatenate([w_key, w_value], axis=1)
    step_rows = block_rows // 3
    cache_spec = pl.BlockSpec((1, step_rows, width), lambda u, b: (u, b, 0))
    new_keys, new_values, part, stat = pl.pallas_call(
        functools.partial(attend_kernel, groups, cap, width ** -0.5),
        grid=(users_here, block_rows // step_rows),
        out_shape=(
            jax.ShapeDtypeStruct(cache_keys.shape, bf16),
            jax.ShapeDtypeStruct(cache_values.shape, bf16),
            jax.ShapeDtypeStruct((blocks, users_here, width, quarter), bf16),
            jax.ShapeDtypeStruct((blocks, users_here, 8, quarter), f32),
        ),
        in_specs=[
            smem, smem, vmem, vmem, cache_spec, cache_spec,
            pl.BlockSpec((blocks, 1, quarter, width), lambda u, b: (0, u, 0, 0)),
        ],
        out_specs=(
            cache_spec, cache_spec,
            pl.BlockSpec((blocks, 1, width, quarter), lambda u, b: (0, u, 0, 0)),
            pl.BlockSpec((blocks, 1, 8, quarter), lambda u, b: (0, u, 0, 0)),
        ),
        scratch_shapes=[
            pltpu.VMEM((groups, cap, 2 * width), bf16),
            pltpu.VMEM((step_rows, 2 * width), f32),
            pltpu.VMEM((blocks, width, quarter), f32),
            pltpu.VMEM((blocks, quarter), f32),
            pltpu.VMEM((blocks, quarter), f32),
            pltpu.VMEM((width, width), bf16),
        ],
        compiler_params=pltpu.CompilerParams(
            dimension_semantics=("arbitrary", "arbitrary"), vmem_limit_bytes=40 * 2**20
        ),
        name="attend",
    )(counts, hist_len, rows, weights, cache_keys, cache_values, queries)

    attended = pl.pallas_call(
        combine_kernel,
        out_shape=jax.ShapeDtypeStruct(candidates.shape, bf16),
        in_specs=[vmem, vmem, smem],
        out_specs=vmem,
        scratch_shapes=[
            pltpu.VMEM((2, users_here, width, quarter), bf16),
            pltpu.VMEM((2, users_here, 8, quarter), f32),
            pltpu.VMEM((users_here, width, quarter), bf16),
            pltpu.VMEM((users_here, 8, quarter), f32),
            pltpu.VMEM((users_here, width, quarter), bf16),
            pltpu.VMEM((users_here, 8, quarter), f32),
            dma((2, 2 * users_here)), dma((2, 2 * users_here)),
            dma((2, users_here)), dma((2, users_here)),
        ],
        compiler_params=pltpu.CompilerParams(collective_id=1, has_side_effects=True),
        name="combine",
    )(part, stat, active)
    return (new_keys, new_values, attended)


def solution(mesh):
    placed = (
        P("user", None),
        P("user"),
        P("user"),
        P(),
        P(),
        P("user", "pos", None),
        P("user", "pos", None),
        P("user"),
        P("user"),
        P("user", "pos", None),
    )
    return jax.shard_map(
        on_device,
        mesh=mesh,
        in_specs=placed,
        out_specs=(P("user", "pos", None), P("user", "pos", None), P("user", "pos", None)),
        check_vma=False,
    )
```

```python
import functools
import math

import jax
import jax.numpy as jnp
from jax import lax
from jax.experimental import pallas as pl
from jax.experimental.pallas import tpu as pltpu
from jax.sharding import PartitionSpec as P

MESH = pl.DeviceIdType.MESH
NT = (((1,), (1,)), ((), ()))
TAIL = 16


def pos_peers():
    p = lax.axis_index("pos")
    near = p + 1 - 2 * lax.rem(p, 2)
    far = lax.rem(p + 2, 4)
    return p, near, far


def merged_kernel(
    groups, blocks, users_here, cap, scale,
    owners_ref, hist_ref, active_ref, events_hbm, cand_hbm, keys_hbm, values_hbm,
    w_key_hbm, w_value_hbm,
    rows_hbm, counts_ref, out_ref,
    events_ref, queries, keys_ref, values_ref, weight_ref, rows_ref, packed, flipped, eye,
    acc, stat, near_out, near_part, near_stat, far_out, far_stat_out, far_part, far_stat,
    load_sem, rows_sem, a2a_send, a2a_recv, hop_send, hop_recv, q_send, q_recv,
    near_send, near_recv, far_send, far_recv,
):
    me = lax.axis_index("user")
    p, near, far = pos_peers()
    low, high = lax.rem(p, 2), p // 2
    cross = 2 * (1 - high) + 1 - low
    count = groups // blocks
    first = lax.rem(p - me + blocks * groups, blocks)
    far_first = lax.rem(far - me + blocks * groups, blocks)
    peers = [first + blocks * k for k in range(count)]
    block_rows, width = keys_ref.shape[1:]
    quarter = queries.shape[2]

    def load(src, dst, n):
        copy = pltpu.make_async_copy(src, dst, load_sem.at[n])
        copy.start()
        return copy

    own_q = load(cand_hbm, queries.at[p], 0)
    events_in = load(events_hbm, events_ref, 1)
    keys_in = load(keys_hbm, keys_ref, 2)
    values_in = load(values_hbm, values_ref, 3)
    weights_in = [load(w_key_hbm, weight_ref.at[0], 4), load(w_value_hbm, weight_ref.at[1], 5)]

    barrier = pltpu.get_barrier_semaphore()
    for peer in (near, far):
        pl.semaphore_signal(barrier, inc=1, device_id={"pos": peer}, device_id_type=MESH)
    for peer in peers:
        @pl.when(peer != me)
        def _():
            pl.semaphore_signal(barrier, inc=1, device_id={"user": peer}, device_id_type=MESH)

    per_event = events_ref.shape[0]
    features = events_ref.shape[1]
    users = groups * users_here
    owner = owners_ref[...]
    user_id = lax.broadcasted_iota(jnp.int32, (users, per_event), 0)
    same = (user_id == owner).astype(jnp.float32)
    before = (
        lax.broadcasted_iota(jnp.int32, (per_event, per_event), 0)
        <= lax.broadcasted_iota(jnp.int32, (per_event, per_event), 1)
    ).astype(jnp.float32).astype(jnp.bfloat16)
    ranks = jnp.dot(same.astype(jnp.bfloat16), before, preferred_element_type=jnp.float32)
    counts = jnp.sum(same, axis=1, keepdims=True)
    dest = owner // users_here
    earlier = (user_id >= dest * users_here) & (user_id < owner)
    slot = jnp.sum(jnp.where(earlier, counts, 0.0) + same * ranks, axis=0, keepdims=True) - 1.0
    slot = slot.astype(jnp.int32)
    slot_id = lax.broadcasted_iota(jnp.int32, (cap, per_event), 0)
    lane = lax.broadcasted_iota(jnp.int32, (users, features), 1)
    lane_user = lax.broadcasted_iota(jnp.int32, (users, features), 0)

    itself = (lax.rem(me, blocks) == first).astype(jnp.int32)
    pl.semaphore_wait(barrier, 2 + count - itself)

    def hop(ref_src, ref_dst, send, recv, peer):
        return pltpu.make_async_remote_copy(
            src_ref=ref_src, dst_ref=ref_dst, send_sem=send, recv_sem=recv,
            device_id={"pos": peer}, device_id_type=MESH,
        )

    own_q.wait()
    q_far = hop(queries.at[p], queries.at[p], q_send.at[0], q_recv.at[0], far)
    q_far.start()
    q_near = hop(queries.at[p], queries.at[p], q_send.at[1], q_recv.at[1], near)
    q_near.start()
    q_across = hop(queries.at[far], queries.at[far], q_send.at[2], q_recv.at[2], near)

    def a2a(k, peer, at):
        return pltpu.make_async_remote_copy(
            src_ref=packed.at[k], dst_ref=rows_ref.at[me],
            send_sem=a2a_send.at[k], recv_sem=a2a_recv.at[at],
            device_id={"user": peer}, device_id_type=MESH,
        )

    def own(k):
        return pltpu.make_async_copy(packed.at[k], rows_ref.at[me], load_sem.at[6 + k])

    events_in.wait()
    for k, peer in enumerate(peers):
        wanted = jnp.where(dest == peer, slot, -1)
        pick = (wanted == slot_id).astype(jnp.float32).astype(jnp.bfloat16)
        packed[k, :cap, :] = jnp.dot(
            pick, events_ref[...], preferred_element_type=jnp.float32
        ).astype(jnp.bfloat16)
        row = jnp.sum(
            jnp.where(lane_user == lane + peer * users_here, counts, 0.0), axis=0, keepdims=True
        )
        packed[k, cap:, :] = jnp.broadcast_to(row, (TAIL, features)).astype(jnp.bfloat16)

        @pl.when(peer != me)
        def _():
            a2a(k, peer, me // blocks).start()

        @pl.when(peer == me)
        def _():
            own(k).start()

    eye[...] = (
        lax.broadcasted_iota(jnp.int32, (width, width), 0)
        == lax.broadcasted_iota(jnp.int32, (width, width), 1)
    ).astype(jnp.float32).astype(jnp.bfloat16)
    factor = scale * math.log2(math.e)
    position = lax.broadcasted_iota(jnp.int32, (block_rows, quarter), 0) + p * block_rows
    keys_in.wait()
    values_in.wait()

    def flip(rows):
        return lax.dot_general(
            eye[...], rows, NT, preferred_element_type=jnp.float32
        ).astype(jnp.bfloat16)

    for u in range(users_here):
        flipped[u] = flip(values_ref[u])

    def keep(c, u, top, total):
        stat[c, u] = jnp.concatenate(
            [jnp.broadcast_to(top, (4, quarter)), jnp.broadcast_to(total, (4, quarter))], axis=0
        )

    def old_part(c):
        def one(u, carry):
            scores = lax.dot_general(
                keys_ref[u], queries[c, u], NT, preferred_element_type=jnp.float32
            ) * factor
            scores = jnp.where(position < hist_ref[u], scores, -1e30)
            top = jnp.maximum(jnp.max(scores, axis=0, keepdims=True), -1e29)
            expo = jnp.exp2(scores - top)
            keep(c, u, top, jnp.sum(expo, axis=0, keepdims=True))
            acc[c, u] = jnp.dot(
                flipped[u], expo.astype(jnp.bfloat16), preferred_element_type=jnp.float32
            )
            return carry

        lax.fori_loop(0, users_here, one, 0)

    old_part(p)
    q_near.wait_recv()
    old_part(near)
    q_far.wait_recv()
    q_across.start()
    old_part(far)
    q_across.wait_recv()
    old_part(cross)

    def forward(stage, k, start, peer):
        block = rows_ref.at[start + blocks * k]
        return hop(block, block, hop_send.at[stage, k], hop_recv.at[stage, k], peer)

    for k, peer in enumerate(peers):
        @pl.when(peer != me)
        def _():
            a2a(k, peer, k).wait_recv()

        @pl.when(peer == me)
        def _():
            own(k).wait()

        forward(0, k, first, far).start()
        forward(1, k, first, near).start()
    for copy in weights_in:
        copy.wait()
    keys_new, flipped_new, masks = [], [], []
    slots = lax.broadcasted_iota(jnp.int32, (cap, quarter), 0).astype(jnp.float32)
    for k, peer in enumerate(peers):
        raw = rows_ref[peer, :cap, :]
        made = [
            jnp.dot(raw, weight_ref[i], preferred_element_type=jnp.float32).astype(jnp.bfloat16)
            for i in range(2)
        ]
        keys_new.append(made[0])
        flipped_new.append(flip(made[1]))
        tail = rows_ref[peer, cap:, :].astype(jnp.float32)
        begin = jnp.zeros((1, 1), jnp.float32)
        mask = []
        for u in range(users_here):
            end = begin + tail[0:1, u : u + 1]
            mask.append((slots >= begin) & (slots < end))
            begin = end
        masks.append(mask)
    keys_new = jnp.concatenate(keys_new, axis=0)
    flipped_new = jnp.concatenate(flipped_new, axis=1)
    masks = [jnp.concatenate([m[u] for m in masks], axis=0) for u in range(users_here)]

    def new_part(c, u):
        scores = lax.dot_general(
            keys_new, queries[c, u], NT, preferred_element_type=jnp.float32
        ) * factor
        scores = jnp.where(masks[u], scores, -1e30)
        old = stat[c, u]
        top = jnp.maximum(jnp.max(scores, axis=0, keepdims=True), old[0:1])
        expo = jnp.exp2(scores - top)
        shrink = jnp.exp2(old[0:1] - top)
        total = old[4:5] * shrink + jnp.sum(expo, axis=0, keepdims=True)
        part = acc[c, u] * shrink + jnp.dot(
            flipped_new, expo.astype(jnp.bfloat16), preferred_element_type=jnp.float32
        )
        return top, total, part

    def copies(pairs, send, recv, n, peer):
        return [
            hop(src, dst, send.at[i, n], recv.at[i, n], peer)
            for i, (src, dst) in enumerate(pairs)
        ]

    first_copies = {}
    for h, c in enumerate((cross, near)):
        for u in range(users_here):
            top, total, part = new_part(c, u)
            near_out[h, u] = part.astype(jnp.bfloat16)
            keep(c, u, top, total)
            first_copies[h, u] = copies(
                ((near_out.at[h, u], near_part.at[h, u]), (stat.at[c, u], near_stat.at[h, u])),
                near_send, near_recv, h * users_here + u, near,
            )
            for copy in first_copies[h, u]:
                copy.start()

    def merge(top, total, part, other, other_part):
        new_top = jnp.maximum(top, other[0:1])
        mine = jnp.exp2(top - new_top)
        theirs = jnp.exp2(other[0:1] - new_top)
        total = total * mine + other[4:5] * theirs
        return new_top, total, part * mine + other_part.astype(jnp.float32) * theirs

    def near_merged(h, c, u):
        top, total, part = new_part(c, u)
        for copy in first_copies[h, u]:
            copy.wait_recv()
        return merge(top, total, part, near_stat[h, u], near_part[h, u])

    second = []
    for u in range(users_here):
        top, total, part = near_merged(0, far, u)
        far_out[u] = part.astype(jnp.bfloat16)
        far_stat_out[u] = jnp.concatenate(
            [jnp.broadcast_to(top, (4, quarter)), jnp.broadcast_to(total, (4, quarter))], axis=0
        )
        second.append(
            copies(
                ((far_out.at[u], far_part.at[u]), (far_stat_out.at[u], far_stat.at[u])),
                far_send, far_recv, u, far,
            )
        )
        for copy in second[u]:
            copy.start()
    for u in range(users_here):
        top, total, part = near_merged(1, p, u)
        acc[p, u] = part
        keep(p, u, top, total)

    for k in range(count):
        forward(0, k, first, far).wait_recv()
        forward(2, k, far_first, near).start()
    for k in range(count):
        forward(1, k, first, near).wait_recv()
        forward(2, k, far_first, near).wait_recv()
    stored = pltpu.make_async_copy(rows_ref, rows_hbm, rows_sem)
    stored.start()
    for g in range(groups):
        counts_ref[g : g + 1, :] = rows_ref[g, cap : cap + TAIL, :128].astype(jnp.float32)[
            0:1
        ].astype(jnp.int32)

    for u in range(users_here):
        for copy in second[u]:
            copy.wait_recv()
        mine = stat[p, u]
        top, total, part = merge(mine[0:1], mine[4:5], acc[p, u], far_stat[u], far_part[u])
        flag = active_ref[u].astype(jnp.float32)
        out_ref[u] = (part * (flag / total)).T.astype(jnp.bfloat16)
    stored.wait()
    for copy in (q_far, q_near, q_across):
        copy.wait_send()
    for group in list(first_copies.values()) + second:
        for copy in group:
            copy.wait_send()
    for k, peer in enumerate(peers):
        @pl.when(peer != me)
        def _():
            a2a(k, peer, k).wait_send()

        forward(0, k, first, far).wait_send()
        forward(1, k, first, near).wait_send()
        forward(2, k, far_first, near).wait_send()


def place_kernel(
    groups, cap,
    count_ref, hist_ref, rows_ref, w_key_ref, w_value_ref, keys_ref, values_ref, attended_ref,
    new_keys_ref, new_values_ref, out_ref,
    made, fresh,
):
    user = pl.program_id(0)
    step = pl.program_id(1)
    steps = pl.num_programs(1)
    rows = keys_ref.shape[1]
    width = keys_ref.shape[2]

    @pl.when((user == 0) & (step == 0))
    def _():
        def project(g, carry):
            for i, weight in enumerate((w_key_ref, w_value_ref)):
                made[g, :, i * width : (i + 1) * width] = jnp.dot(
                    rows_ref[g, :cap, :], weight[...], preferred_element_type=jnp.float32
                ).astype(jnp.bfloat16)
            return carry

        lax.fori_loop(0, groups, project, 0)

    out_ref[...] = attended_ref[...]
    origin = (lax.axis_index("pos") * steps + step) * rows
    start = hist_ref[user] - origin
    limit = lax.fori_loop(0, groups, lambda g, n: n + count_ref[g, user], start)
    touched = (limit > 0) & (start < rows) & (limit > start)

    @pl.when(jnp.logical_not(touched))
    def _():
        new_keys_ref[...] = keys_ref[...]
        new_values_ref[...] = values_ref[...]

    @pl.when(touched)
    def _():
        fresh[...] = jnp.zeros_like(fresh)
        gap = lax.broadcasted_iota(jnp.int32, (rows, cap), 1) - lax.broadcasted_iota(
            jnp.int32, (rows, cap), 0
        )
        slot = lax.broadcasted_iota(jnp.int32, (rows, cap), 1)

        def place(g, at):
            size = count_ref[g, user]

            @pl.when((size > 0) & (at < rows) & (at + size > 0))
            def _():
                low = lax.fori_loop(0, user, lambda j, n: n + count_ref[g, j], 0)
                pick = (gap == low - at) & (slot >= low) & (slot < low + size)
                fresh[...] += jnp.dot(
                    pick.astype(jnp.float32).astype(jnp.bfloat16), made[g],
                    preferred_element_type=jnp.float32,
                )

            return at + size

        lax.fori_loop(0, groups, place, start)
        row = lax.broadcasted_iota(jnp.int32, (rows, width), 0)
        inside = (row >= start) & (row < limit)
        new_keys_ref[0] = jnp.where(
            inside, fresh[:, :width], keys_ref[0].astype(jnp.float32)
        ).astype(jnp.bfloat16)
        new_values_ref[0] = jnp.where(
            inside, fresh[:, width:], values_ref[0].astype(jnp.float32)
        ).astype(jnp.bfloat16)


def on_device(
    events, owners, offsets, w_key, w_value, cache_keys, cache_values, hist_len, active, candidates
):
    groups = lax.axis_size("user")
    blocks = lax.axis_size("pos")
    users_here, block_rows, width = cache_keys.shape
    per_event, features = events.shape
    cap = 2 * per_event // groups
    quarter = candidates.shape[1]
    count = groups // blocks
    vmem = pl.BlockSpec(memory_space=pltpu.VMEM)
    smem = pl.BlockSpec(memory_space=pltpu.SMEM)
    hbm = pl.BlockSpec(memory_space=pl.ANY)
    dma = pltpu.SemaphoreType.DMA
    bf16, f32 = jnp.bfloat16, jnp.float32

    rows, counts, attended = pl.pallas_call(
        functools.partial(merged_kernel, groups, blocks, users_here, cap, width ** -0.5),
        out_shape=(
            jax.ShapeDtypeStruct((groups, cap + TAIL, features), bf16),
            jax.ShapeDtypeStruct((groups, 128), jnp.int32),
            jax.ShapeDtypeStruct(candidates.shape, bf16),
        ),
        in_specs=[vmem, smem, smem] + [hbm] * 6,
        out_specs=(hbm, vmem, vmem),
        scratch_shapes=[
            pltpu.VMEM(events.shape, bf16),
            pltpu.VMEM((blocks,) + candidates.shape, bf16),
            pltpu.VMEM(cache_keys.shape, bf16),
            pltpu.VMEM(cache_values.shape, bf16),
            pltpu.VMEM((2, features, width), bf16),
            pltpu.VMEM((groups, cap + TAIL, features), bf16),
            pltpu.VMEM((count, cap + TAIL, features), bf16),
            pltpu.VMEM((users_here, width, block_rows), bf16),
            pltpu.VMEM((width, width), bf16),
            pltpu.VMEM((blocks, users_here, width, quarter), f32),
            pltpu.VMEM((blocks, users_here, 8, quarter), f32),
            pltpu.VMEM((2, users_here, width, quarter), bf16),
            pltpu.VMEM((2, users_here, width, quarter), bf16),
            pltpu.VMEM((2, users_here, 8, quarter), f32),
            pltpu.VMEM((users_here, width, quarter), bf16),
            pltpu.VMEM((users_here, 8, quarter), f32),
            pltpu.VMEM((users_here, width, quarter), bf16),
            pltpu.VMEM((users_here, 8, quarter), f32),
            dma((6 + count,)), dma, dma((count,)), dma((count,)),
            dma((3, count)), dma((3, count)), dma((3,)), dma((3,)),
            dma((2, 2 * users_here)), dma((2, 2 * users_here)),
            dma((2, users_here)), dma((2, users_here)),
        ],
        compiler_params=pltpu.CompilerParams(
            collective_id=0, has_side_effects=True, vmem_limit_bytes=60 * 2**20
        ),
        name="merged",
    )(
        owners.reshape(1, per_event), hist_len, active, events, candidates,
        cache_keys, cache_values, w_key, w_value,
    )

    step_rows = block_rows // 3
    cache_spec = pl.BlockSpec((1, step_rows, width), lambda u, b: (u, b, 0))
    read_spec = pl.BlockSpec((1, quarter, width), lambda u, b: (u, 0, 0))
    return pl.pallas_call(
        functools.partial(place_kernel, groups, cap),
        grid=(users_here, block_rows // step_rows),
        out_shape=(
            jax.ShapeDtypeStruct(cache_keys.shape, bf16),
            jax.ShapeDtypeStruct(cache_values.shape, bf16),
            jax.ShapeDtypeStruct(candidates.shape, bf16),
        ),
        in_specs=[smem, smem, vmem, vmem, vmem, cache_spec, cache_spec, read_spec],
        out_specs=(cache_spec, cache_spec, read_spec),
        scratch_shapes=[
            pltpu.VMEM((groups, cap, 2 * width), bf16),
            pltpu.VMEM((step_rows, 2 * width), f32),
        ],
        compiler_params=pltpu.CompilerParams(
            dimension_semantics=("arbitrary", "arbitrary"), vmem_limit_bytes=60 * 2**20
        ),
        name="place",
    )(counts, hist_len, rows, w_key, w_value, cache_keys, cache_values, attended)


def solution(mesh):
    placed = (
        P("user", None),
        P("user"),
        P("user"),
        P(),
        P(),
        P("user", "pos", None),
        P("user", "pos", None),
        P("user"),
        P("user"),
        P("user", "pos", None),
    )
    return jax.shard_map(
        on_device,
        mesh=mesh,
        in_specs=placed,
        out_specs=(P("user", "pos", None), P("user", "pos", None), P("user", "pos", None)),
        check_vma=False,
    )
```
